32 devices in a mesh: groups: 2 (over y), expert: 8 (over z, core), tensor: 2 (over x).
Axes of the slice: x: 2, y: 2, z: 4, core: 2. Of those that a mesh axis runs over, the one named last changes fastest.
Arguments:
- queries: bfloat16 [512, 4096], P(('groups', 'expert')), parts along dimension 0, may hold values from -200 to 200
- own_kv: bfloat16 [512, 1024], P(('groups', 'expert')), parts along dimension 0, may hold values from -6 to 6
- prompt_cache: bfloat16 [16, 256, 1024], P(('groups', 'expert'), 'tensor'), parts along dimension 0, may hold values from -8 to 8
- prompt_len: int32 [16], P(('groups', 'expert')), parts along dimension 0, may hold values from 2 to 256
- token_prompt: int32 [512], P(('groups', 'expert')), parts along dimension 0, may hold values from 0 to 7, as said below
- residual: bfloat16 [512, 2048], P(('groups', 'expert')), parts along dimension 0, may hold values from -3 to 3
- out_weight: bfloat16 [4096, 2048], P('tensor', 'expert'), may hold values from -0.125 to 0.125
- route_ids: int32 [512, 8], P(('groups', 'expert')), parts along dimension 0, may hold values from 0 to 15, all different within a row; in each aligned block of 32 rows (0 to 31, 32 to 63, ...) at most 24 rows name the same one
- route_weights: float32 [512, 8], P(('groups', 'expert')), parts along dimension 0, may hold values from 0.05 to 0.3
- w_gate: bfloat16 [16, 2048, 1024], P('expert', None, 'tensor'), may hold values from -0.125 to 0.125
- w_up: bfloat16 [16, 2048, 1024], P('expert', None, 'tensor'), may hold values from -0.125 to 0.125
- w_down: bfloat16 [16, 1024, 2048], P('expert', 'tensor'), may hold values from -0.25 to 0.25
Outputs:
- mixed: bfloat16 [512, 2048], P(('groups', 'expert'), 'tensor'), parts along dimension 0
The draws below stay inside these ranges and needn't reach their ends.
There are 2 independent parts, one for each index of `groups`. The reference program is written for one: setup_inputs(seed, part) draws one part's arguments, and reference() takes and returns one part's arrays. A program takes and returns all parts, laid end to end along the dimension named above; an argument that names none is the same for every part. Nothing has to cross between parts.
Inputs may be any that keep to these rules, and one draw needn't show every extreme that they name: `token_prompt`: each index of the expert axis holds 8 tokens of each of 4 prompts and none of the others; each prompt has tokens on exactly 4 indices. `route_ids`: A row names distinct experts. Within the 32 rows of one index of the expert axis no expert is named more than 24 times, and in some of these blocks one is named exactly 24 times.
All inputs are finite; a program needn't handle non-finite values.
Results may differ from the reference program's by a relative error of at most 0.015.
Values may be sent and summed in bfloat16 or wider, within the bound.
A program may use at most 64 MiB of HBM per device.

```python
import math
import jax
import jax.numpy as jnp
import numpy as np
from jax import lax

D = 2048
H = 32
KVH = 4
HD = 128
FF = 1024
TOPK = 8
P_SIZE = 256
TOK_DEV = 32
E = 16
NPROMPT = 8
FAN = 4
TOKENS = 256
CAP = 24
FF_DEV = 512
N_EXPERT = 8
N_TENSOR = 2


def prompt_table(key):
    base = jax.random.fold_in(key, 11)
    key_one, key_two, key_three = jax.random.split(base, 3)
    order_a = jax.random.permutation(key_one, NPROMPT)
    order_b = jax.random.permutation(key_two, NPROMPT)
    inverse_a = jnp.argsort(order_a)
    offsets = jnp.tile(jnp.arange(TOK_DEV, dtype=jnp.int32) % FAN, (NPROMPT, 1))
    offsets = jax.random.permutation(key_three, offsets, axis=1, independent=True)
    chosen = (order_b[:, None] + offsets) % NPROMPT
    return inverse_a[chosen].reshape(-1).astype(jnp.int32)


def cache_table(key):
    base = jax.random.fold_in(key, 23)
    key_main = jax.random.fold_in(base, 0)
    cache_vals = jnp.clip(jax.random.normal(key_main, (NPROMPT, P_SIZE, 2 * KVH * HD), jnp.float32), -6.0, 6.0)
    return cache_vals


def draw_token_prompt(key, part):
    return prompt_table(key)


def draw_prompt_cache(key, part):
    return cache_table(key).astype(jnp.bfloat16)


def draw_queries(key, part):
    base = jax.random.fold_in(key, 37)
    key_main = jax.random.fold_in(base, 0)
    values = jnp.clip(jax.random.normal(key_main, (TOKENS, H * HD), jnp.float32), -6.0, 6.0)
    return values.astype(jnp.bfloat16)


def touch_ends(result, key, smallest, high):
    spot = [jax.random.randint(jax.random.fold_in(key, axis), (), 0, length) for axis, length in enumerate(result.shape)]
    main_axis = result.shape.index(max(result.shape))
    neighbour = spot[:main_axis] + [(spot[main_axis] + 1) % result.shape[main_axis]] + spot[main_axis + 1:]
    return result.at[tuple(spot)].set(smallest).at[tuple(neighbour)].set(high)


def with_spikes(values, own_key, source, target, parts, factor):
    owner, partner = [(jnp.arange(values.shape[axis_at]) // (values.shape[axis_at] // parts)).reshape([-1 if axis == axis_at else 1 for axis in range(values.ndim)]) for axis_at in (source, target)]
    chosen = jax.random.permutation(own_key, parts)[partner]
    strong = (owner == chosen) | (owner == (partner + parts // 2) % parts)
    return jnp.where(strong, factor * values, values)


def shard_levels(key, extent, cuts, low, top_value):
    level, own = 1.0, jax.random.fold_in(key, 6)
    for axis_at, parts in cuts:
        draws = jnp.exp(jax.random.uniform(jax.random.fold_in(own, axis_at), (parts,), jnp.float32, low / len(cuts), top_value / len(cuts)))
        level = level * jnp.repeat(draws, extent[axis_at] // parts).reshape([-1 if axis == axis_at else 1 for axis in range(len(extent))])
    return level


def assign_block(own_key, own, number, rows, count, top, limit, slope):
    order = jax.random.permutation(own_key, count)
    heavy_load, common = portions_of(count, rows * top, limit, slope, True), portions_of(count, rows * top, limit, slope, False)
    places = jnp.arange(count)

    def named(sizes, offset_by):
        used = int((sizes > 0).sum())
        fixed = max(1, used // 4)
        moved = fixed + (places - fixed + offset_by * (used - fixed)) % max(1, count - fixed)
        return jnp.zeros((count,), jnp.int32).at[order[jnp.where(places < fixed, places, moved)]].set(jnp.asarray(sizes, jnp.int32))

    sizes = jnp.where(number % 4 == 0, named(heavy_load, number // 4), named(common, number - number // 4 - 1))
    mixed = jax.random.permutation(jax.random.fold_in(own, 3), count)
    giver, sink = mixed[0:count // 2 * 2:2], mixed[1:count // 2 * 2:2]
    room = jnp.minimum(sizes[giver] - 1, limit - sizes[sink]) // 2
    room = jnp.where((giver == order[0]) | (sink == order[0]) | (sizes[sink] == 0), 0, jnp.maximum(room, 0))
    moved = jax.random.randint(jax.random.fold_in(own, 4), (count // 2,), 0, 1 << 20) % (room + 1)
    sizes = sizes.at[giver].add(-moved).at[sink].add(moved)
    labels = jnp.searchsorted(jnp.cumsum(sizes), jnp.arange(rows * top), side="right").astype(jnp.int32)
    grid = labels.reshape(top, rows).T
    grid = grid[jax.random.permutation(jax.random.fold_in(own, 1), rows)]
    offset_by = jax.random.randint(jax.random.fold_in(own, 2), (rows, 1), 0, top)
    return jnp.take_along_axis(grid, (jnp.arange(top)[None, :] + offset_by) % top, axis=1)


def portions_of(number_of, total, reach, slope, full):
    loads = [(1 << 20) // math.isqrt(grade ** slope) + 1 for grade in range(1, number_of + 1)]
    largest = reach if full else min(reach, max(-(-total // number_of), total * loads[0] // sum(loads)))
    least = 1 if total - largest >= number_of - 1 else 0
    holding, rest = [largest] + [least] * (number_of - 1), total - largest - least * (number_of - 1)
    while rest > 0:
        free = [i for i in range(1, number_of) if holding[i] < largest] or [i for i in range(1, number_of) if holding[i] < reach]
        mass, remaining = sum([loads[i] for i in free]), rest
        for i in free:
            extra = min(reach - holding[i], max(1, remaining * loads[i] // mass), rest)
            holding[i] = holding[i] + extra
            rest = rest - extra
    return np.array(holding)


def normal_values(stream_key, shape, deviation, limit, cuts=(), held_as=jnp.bfloat16):
    result = jax.random.normal(stream_key, shape, jnp.float32) * deviation
    if len(cuts) > 0:
        result = shard_levels(stream_key, shape, cuts, -0.22, 0.18) * result
    return jnp.clip(result, min=-limit, max=limit).astype(held_as)


def noise_with(stream_key, dims, deviation, reach, cuts, heavy, kind=jnp.bfloat16):
    values = deviation * jax.random.normal(stream_key, dims, jnp.float32)
    if cuts:
        values = values * shard_levels(stream_key, dims, cuts, -0.22, 0.18)
    return jnp.clip(with_spikes(values, jax.random.fold_in(stream_key, 3), *heavy), -reach, reach).astype(kind)


def setup_inputs(seed: int = 0, part: int = 0) -> dict:
    arg_keys = jax.random.split(jax.random.key(seed), 13)
    part_keys = jax.random.split(jax.random.fold_in(arg_keys[12], part), 13)
    queries = draw_queries(jax.random.fold_in(jax.random.fold_in(arg_keys[12], part), 71), part)
    own_kv = normal_values(part_keys[1], (TOKENS, 2 * KVH * HD), 1.0, 6.0, ((0, 8),))
    prompt_cache = draw_prompt_cache(jax.random.fold_in(jax.random.fold_in(arg_keys[12], part), 71), part)
    prompt_len = touch_ends(jax.random.randint(part_keys[3], (NPROMPT,), 2, P_SIZE + 1), jax.random.fold_in(part_keys[3], 1), 2, P_SIZE).astype(jnp.int32)
    token_prompt = draw_token_prompt(jax.random.fold_in(jax.random.fold_in(arg_keys[12], part), 71), part)
    residual = normal_values(part_keys[5], (TOKENS, D), 0.5, 3.0, ((0, 8),))
    out_weight = noise_with(arg_keys[6], (H * HD, D), (H * HD) ** -0.5, 0.125, ((0, 2), (1, 8)), (0, 1, 8, 2.0))
    route_ids_keys = jax.random.split(jax.random.fold_in(part_keys[7], 1), TOKENS // TOK_DEV)
    route_ids_turns = jax.random.permutation(jax.random.fold_in(part_keys[7], 3), TOKENS // TOK_DEV)
    route_ids = jax.vmap(lambda own, number: assign_block(jax.random.fold_in(part_keys[7], 2), own, number, TOK_DEV, E, TOPK, CAP, 2))(route_ids_keys, route_ids_turns).reshape((TOKENS, TOPK))
    route_weights = jnp.clip(0.05 + 0.25 * jax.random.uniform(part_keys[8], (TOKENS, TOPK), jnp.float32) ** shard_levels(part_keys[8], (TOKENS, TOPK), ((0, 8),), -0.2, 0.2), 0.05, 0.3)
    w_gate = normal_values(arg_keys[9], (E, D, FF), D ** -0.5, 0.125, ((0, 8), (2, 2)))
    w_up = normal_values(arg_keys[10], (E, D, FF), D ** -0.5, 0.125, ((0, 8), (2, 2)))
    w_down = noise_with(arg_keys[11], (E, FF, D), FF ** -0.5, 0.25, ((0, 8), (1, 2)), (1, 2, 2, 2.0))
    return dict(queries=queries, own_kv=own_kv, prompt_cache=prompt_cache, prompt_len=prompt_len, token_prompt=token_prompt, residual=residual, out_weight=out_weight, route_ids=route_ids, route_weights=route_weights, w_gate=w_gate, w_up=w_up, w_down=w_down)


MASKED_SCORE = -1e30


def prompt_attention(inputs):
    query_rows, own_keys, own_values, key_rows, value_rows, length = inputs
    score_scale = HD ** -0.5
    score_rows = jnp.einsum('tgjd,pgd->tgjp', query_rows, key_rows, precision=lax.Precision.HIGHEST) * score_scale
    visible = jnp.arange(P_SIZE) < length
    score_rows = jnp.where(visible, score_rows, MASKED_SCORE)
    own_score = jnp.einsum('tgjd,tgd->tgj', query_rows, own_keys, precision=lax.Precision.HIGHEST) * score_scale
    top_score = jnp.maximum(jnp.max(score_rows, -1), own_score)
    weights = jnp.where(visible, jnp.exp(score_rows - top_score[..., None]), 0.0)
    own_weight = jnp.exp(own_score - top_score)
    weight_sum = jnp.sum(weights, -1) + own_weight
    value_sum = jnp.einsum('tgjp,pgd->tgjd', weights, value_rows, precision=lax.Precision.HIGHEST)
    value_sum = value_sum + own_weight[..., None] * own_values[:, :, None, :]
    return value_sum / weight_sum[..., None]


def expert_layer(inputs):
    rows_in, gate_weight, up_weight, down_weight = inputs
    gate_proj = jnp.dot(rows_in, gate_weight, preferred_element_type=jnp.float32)
    up_proj = jnp.dot(rows_in, up_weight, preferred_element_type=jnp.float32)
    activated = (jax.nn.silu(gate_proj) * up_proj).astype(jnp.bfloat16)
    row_count = rows_in.shape[0]
    act_blocks = activated.astype(jnp.float32).reshape(row_count, N_TENSOR, FF_DEV)
    down_blocks = down_weight.astype(jnp.float32).reshape(N_TENSOR, FF_DEV, D)
    partials = jnp.einsum('rnf,nfd->nrd', act_blocks, down_blocks, precision=lax.Precision.HIGHEST)
    partials = partials.astype(jnp.bfloat16).astype(jnp.float32)
    return jnp.sum(partials, 0).astype(jnp.bfloat16)


def reference(queries, own_kv, prompt_cache, prompt_len, token_prompt, residual, out_weight, route_ids, route_weights, w_gate, w_up, w_down):
    group_size = H // KVH
    half_cols = KVH * HD
    order = jnp.argsort(token_prompt, stable=True).astype(jnp.int32)
    grouped = order.reshape(NPROMPT, TOK_DEV)
    query_all = queries.astype(jnp.float32).reshape(TOKENS, KVH, group_size, HD)
    own_all = own_kv.astype(jnp.float32)
    own_keys = own_all[:, :half_cols].reshape(TOKENS, KVH, HD)
    own_values = own_all[:, half_cols:].reshape(TOKENS, KVH, HD)
    cache_all = prompt_cache.astype(jnp.float32)
    key_rows = cache_all[:, :, :half_cols].reshape(NPROMPT, P_SIZE, KVH, HD)
    value_rows = cache_all[:, :, half_cols:].reshape(NPROMPT, P_SIZE, KVH, HD)
    results = lax.map(prompt_attention, (query_all[grouped], own_keys[grouped], own_values[grouped], key_rows, value_rows, prompt_len))
    attn = jnp.zeros((TOKENS, H * HD), jnp.float32).at[order].set(results.reshape(TOKENS, H * HD)).astype(jnp.bfloat16)
    attn_out = jnp.dot(attn, out_weight, preferred_element_type=jnp.float32)
    hidden = (residual.astype(jnp.float32) + attn_out).astype(jnp.bfloat16)

    flat_ids = route_ids.reshape(N_EXPERT, TOK_DEV * TOPK)
    expert_marks = (flat_ids[..., None] == jnp.arange(E, dtype=jnp.int32)).astype(jnp.int32)
    slot_index = jnp.sum((jnp.cumsum(expert_marks, 1) - expert_marks) * expert_marks, -1).astype(jnp.int32)
    destination = (flat_ids * CAP + slot_index).astype(jnp.int32)
    source_rows = (jnp.arange(TOK_DEV * TOPK) // TOPK).astype(jnp.int32)
    block_ids = jnp.arange(N_EXPERT, dtype=jnp.int32)[:, None]
    hidden_blocks = hidden.reshape(N_EXPERT, TOK_DEV, D)
    buffers = jnp.zeros((N_EXPERT, E * CAP, D), jnp.bfloat16)
    buffers = buffers.at[block_ids, destination].set(hidden_blocks[block_ids, source_rows[None, :]])
    expert_in = buffers.reshape(N_EXPERT, E, CAP, D).transpose(1, 0, 2, 3).reshape(E, N_EXPERT * CAP, D)
    expert_out = lax.map(expert_layer, (expert_in, w_gate, w_up, w_down)).reshape(E, N_EXPERT, CAP, D)
    picked = expert_out[flat_ids, block_ids, slot_index].reshape(TOKENS, TOPK, D).astype(jnp.float32)
    expert_mix = jnp.sum(route_weights[:, :, None] * picked, 1)
    return (hidden.astype(jnp.float32) + expert_mix).astype(jnp.bfloat16)
```

```python
import functools

import jax
import jax.numpy as jnp
from jax import lax
from jax.experimental import pallas as pl
from jax.experimental.pallas import tpu as pltpu
from jax.sharding import PartitionSpec as P

HD = 128


MASKED_SCORE = -1e30


def combined_all(x, axis, combine):
    everything = jax.tree.map(
        lambda part, kind: lax.all_gather(part.astype(kind), axis),
        x,
        jax.tree.map(lambda a: jnp.bfloat16 if a.dtype == jnp.float32 else a.dtype, x),
    )

    def take(k):
        return jax.tree.map(lambda part, own: part[k].astype(own.dtype), everything, x)

    return lax.fori_loop(
        1, lax.axis_size(axis), lambda k, so_far: combine(so_far, take(k)), take(0)
    )


def combine_parts(earlier, later):
    top_a, sum_a, value_a = earlier
    top_b, sum_b, value_b = later
    top_score = jnp.maximum(top_a, top_b)
    shrink_a = jnp.exp(top_a - top_score)
    shrink_b = jnp.exp(top_b - top_score)
    return (
        top_score,
        sum_a * shrink_a + sum_b * shrink_b,
        value_a * shrink_a[..., None] + value_b * shrink_b[..., None],
    )


def local(
    queries,
    own_kv,
    prompt_cache,
    prompt_len,
    token_prompt,
    residual,
    out_weight,
    route_ids,
    route_weights,
    w_gate,
    w_up,
    w_down,
):
    tokens = queries.shape[0]
    half_cols = own_kv.shape[1] // 2
    kv_heads = half_cols // HD
    head_count = queries.shape[1] // HD
    group_size = head_count // kv_heads
    score_scale = HD ** (-0.5)
    expert_groups = lax.axis_size("expert")
    fan_count = expert_groups // 2
    per_prompt = tokens // fan_count
    order = jnp.argsort(token_prompt, stable=True)
    inverse = jnp.argsort(order)
    held_prompts = token_prompt[order].reshape(fan_count, per_prompt)[:, 0]
    sorted_query = queries[order].reshape(fan_count, per_prompt, kv_heads, group_size, HD)
    sorted_own = own_kv[order]
    own_keys = sorted_own[:, :half_cols].reshape(fan_count, per_prompt, kv_heads, HD)
    own_values = (
        sorted_own[:, half_cols:].reshape(fan_count, per_prompt, kv_heads, HD).astype(jnp.float32)
    )
    own_score = (
        jnp.einsum("imgjd,imgd->imgj", sorted_query, own_keys, preferred_element_type=jnp.float32)
        * score_scale
    )
    tensor_pos = lax.axis_index("tensor")
    leading = tensor_pos == 0
    start_top = jnp.where(leading, own_score, MASKED_SCORE)
    start_sum = jnp.where(leading, jnp.ones_like(own_score), jnp.zeros_like(own_score))
    start_values = jnp.where(
        leading,
        jnp.broadcast_to(
            own_values[:, :, :, None, :], (fan_count, per_prompt, kv_heads, group_size, HD)
        ),
        0.0,
    )
    block_len = prompt_cache.shape[1]
    positions = tensor_pos * block_len + jnp.arange(block_len, dtype=jnp.int32)
    cache_piece = lax.all_gather(prompt_cache, "expert", axis=0, tiled=True)
    length_piece = lax.all_gather(prompt_len, "expert", axis=0, tiled=True)
    shard_count = cache_piece.shape[0]
    owners = jnp.arange(shard_count, dtype=jnp.int32)
    matched = owners[:, None] == held_prompts[None, :]
    match_half = matched.astype(jnp.bfloat16)
    match_full = matched.astype(jnp.float32)
    present = jnp.any(matched, 0)
    piece_query = jnp.einsum(
        "qi,imgjd->qmgjd", match_half, sorted_query, preferred_element_type=jnp.float32
    ).astype(jnp.bfloat16)
    key_rows = cache_piece[:, :, :half_cols].reshape(shard_count, block_len, kv_heads, HD)
    value_rows = (
        cache_piece[:, :, half_cols:]
        .reshape(shard_count, block_len, kv_heads, HD)
        .astype(jnp.float32)
    )
    inside = (positions[None, :] < length_piece[:, None])[:, None, None, None, :]
    score_rows = (
        jnp.einsum("qmgjd,qpgd->qmgjp", piece_query, key_rows, preferred_element_type=jnp.float32)
        * score_scale
    )
    score_rows = jnp.where(inside, score_rows, MASKED_SCORE)
    piece_top = jnp.max(score_rows, -1)
    weights = jnp.where(inside, jnp.exp(score_rows - piece_top[..., None]), 0.0)
    piece_sum = jnp.sum(weights, -1)
    piece_values = jnp.einsum(
        "qmgjp,qpgd->qmgjd", weights, value_rows, precision=lax.Precision.HIGHEST
    )
    group_top = jnp.einsum("qi,qmgj->imgj", match_full, piece_top, precision=lax.Precision.HIGHEST)
    group_top = jnp.where(present[:, None, None, None], group_top, MASKED_SCORE)
    group_sum = jnp.einsum("qi,qmgj->imgj", match_full, piece_sum, precision=lax.Precision.HIGHEST)
    group_values = jnp.einsum(
        "qi,qmgjd->imgjd", match_full, piece_values, precision=lax.Precision.HIGHEST
    )
    folded = combine_parts(
        (start_top, start_sum, start_values), (group_top, group_sum, group_values)
    )
    top_score, weight_sum, value_sum = combined_all(folded, "tensor", combine_parts)
    attn_sorted = (value_sum / weight_sum[..., None]).reshape(tokens, head_count * HD)
    attn = attn_sorted[inverse].astype(jnp.bfloat16)
    rows_here = out_weight.shape[0]
    attn_mine = lax.dynamic_slice_in_dim(attn, tensor_pos * rows_here, rows_here, 1)
    column_terms = jnp.dot(
        lax.all_gather(attn_mine, "expert", axis=0, tiled=True),
        out_weight,
        preferred_element_type=jnp.float32,
    )
    partials = lax.all_to_all(
        column_terms.astype(jnp.bfloat16), "expert", split_axis=0, concat_axis=1, tiled=True
    ).astype(column_terms.dtype)
    model_width = residual.shape[1]
    col_width = model_width // lax.axis_size("tensor")
    col_start = tensor_pos * col_width
    resid_cols = lax.dynamic_slice_in_dim(residual, col_start, col_width, 1)
    experts_here = w_gate.shape[0]
    experts = experts_here * expert_groups
    picks = route_ids.shape[1]
    capacity = min(tokens, 3 * tokens * picks // (2 * experts))
    flat_ids = route_ids.reshape(-1)
    expert_marks = (flat_ids[:, None] == jnp.arange(experts, dtype=jnp.int32)[None, :]).astype(
        jnp.int32
    )
    slot_index = jnp.sum((jnp.cumsum(expert_marks, 0) - expert_marks) * expert_marks, 1)
    destination = flat_ids * capacity + slot_index
    source_rows = jnp.arange(tokens * picks, dtype=jnp.int32) // picks
    head_total = lax.psum_scatter(
        partials.astype(jnp.bfloat16), "tensor", scatter_dimension=1, tiled=True
    ).astype(jnp.float32)
    hidden_cols = (resid_cols.astype(jnp.float32) + head_total).astype(jnp.bfloat16)
    outgoing = (
        jnp.zeros((experts * capacity, col_width), jnp.bfloat16)
        .at[destination]
        .set(hidden_cols[source_rows])
    )
    outgoing = outgoing.reshape(expert_groups, experts_here, capacity, col_width)
    arrived = lax.all_to_all(outgoing, "expert", split_axis=0, concat_axis=0, tiled=True)
    arrived = lax.all_gather(arrived, "tensor", axis=3, tiled=True)
    gate_proj = jnp.einsum("sxcd,xdf->sxcf", arrived, w_gate, preferred_element_type=jnp.float32)
    up_proj = jnp.einsum("sxcd,xdf->sxcf", arrived, w_up, preferred_element_type=jnp.float32)
    activated = (jax.nn.silu(gate_proj) * up_proj).astype(jnp.bfloat16)
    expert_partials = jnp.einsum(
        "sxcf,xfd->sxcd", activated, w_down, preferred_element_type=jnp.float32
    )
    summed = lax.psum_scatter(
        expert_partials.astype(jnp.bfloat16), "tensor", scatter_dimension=3, tiled=True
    )
    returned = lax.all_to_all(summed, "expert", split_axis=0, concat_axis=0, tiled=True).reshape(
        experts * capacity, col_width
    )
    picked = returned[destination].reshape(tokens, picks, col_width).astype(jnp.float32)
    expert_mix = jnp.sum(route_weights[:, :, None] * picked, 1)
    return (hidden_cols.astype(jnp.float32) + expert_mix).astype(jnp.bfloat16)


F32 = jnp.float32
BF16 = jnp.bfloat16
MESH = pl.DeviceIdType.MESH


def dot(a, b):
    return jnp.dot(a, b, preferred_element_type=F32)


def iota(shape, dim):
    return lax.broadcasted_iota(jnp.int32, shape, dim)


def fused_kernel(
    sizes,
    queries_hbm,
    own_kv_hbm,
    cache,
    length_hbm,
    tp_hbm,
    residual,
    ids_hbm,
    route_w_hbm,
    wo_hbm,
    wg_hbm,
    wu_hbm,
    wd_hbm,
    out,
    queries,
    own_kv,
    length,
    tp_row,
    ids,
    route_w,
    wo,
    wg,
    wu,
    wd,
    qsend,
    qrecv,
    kv,
    msend,
    meta,
    resid,
    sorted_resid,
    perm,
    mixes,
    attn,
    ybuf,
    yrecv,
    hidden,
    act,
    own_act,
    total,
    dsend,
    drecv,
    xsend,
    xrecv,
    zsend,
    zrecv,
    in_sem,
    w_sem,
    q_ss,
    q_rs,
    m_ss,
    m_rs,
    r_ss,
    r_rs,
    k_ss,
    k_rs,
    a_ss,
    a_rs,
    m_up_ss,
    m_up_rs,
    y_ss,
    y_rs,
    h_ss,
    h_rs,
    d_ss,
    d_rs,
    x_ss,
    x_rs,
    z_ss,
    z_rs,
):
    n, tokens, per, kvl, group = sizes
    nz = n // 2
    me = lax.axis_index("expert")
    t = lax.axis_index("tensor")
    ot = 1 - t
    z = me // 2
    c = lax.rem(me, 2)
    mate = z * 2 + 1 - c
    everyone = n * tokens
    model = residual.shape[1]
    cols = model // n
    hc = cols // 2
    half = model // 2
    heads_cols = kvl * group * HD
    block_cols = group * HD + 2 * HD
    half_kv = own_kv.shape[1] // 2
    experts_here = wg.shape[0]
    ff = wg.shape[2]

    step = 2 * (z // (nz // 2)) - 1

    def zline(k):
        return lax.rem(z + nz + step * k, nz)

    def peer(k):
        return zline(k // 2) * 2 + lax.rem(c + k, 2)

    def zpeer(k):
        return zline(k) * 2 + c

    def slot(b):
        return lax.rem(b + n - 2, n)

    def mult(x, m):
        return pl.multiple_of(x, m)

    loads = [
        pltpu.make_async_copy(a, b, w_sem.at[i])
        for i, (a, b) in enumerate(((wo_hbm, wo), (wg_hbm, wg), (wu_hbm, wu), (wd_hbm, wd)))
    ]
    fetched = [
        pltpu.make_async_copy(a, b, in_sem.at[i])
        for i, (a, b) in enumerate(
            (
                (tp_hbm, tp_row),
                (queries_hbm, queries),
                (own_kv_hbm, own_kv),
                (ids_hbm, ids),
                (route_w_hbm, route_w),
                (length_hbm, length),
            )
        )
    ]
    for fetch in fetched:
        fetch.start()

    barrier = pltpu.get_barrier_semaphore()
    for k in range(1, n):
        pl.semaphore_signal(
            barrier, inc=1, device_id={"expert": peer(k), "tensor": t}, device_id_type=MESH
        )
    pl.semaphore_signal(
        barrier, inc=1, device_id={"expert": me, "tensor": ot}, device_id_type=MESH
    )

    def remote(src, dst, ss, rs, e, tt):
        return pltpu.make_async_remote_copy(
            src_ref=src,
            dst_ref=dst,
            send_sem=ss,
            recv_sem=rs,
            device_id={"expert": e, "tensor": tt},
            device_id_type=MESH,
        )

    kvw = kvl * HD
    span = cache.shape[1]
    mine_at = pl.ds(mult(t * span, span), span)
    own_half = [
        pltpu.make_async_copy(
            cache.at[0, :, pl.ds(mult(i * half_kv + t * kvw, kvw), kvw)],
            kv.at[mine_at, pl.ds(i * kvw, kvw)],
            in_sem.at[6 + i],
        )
        for i in range(2)
    ]
    own_half.append(
        pltpu.make_async_copy(
            residual.at[:, pl.ds(mult(me * cols + t * hc, hc), hc)], resid.at[me], in_sem.at[8]
        )
    )
    for load in own_half:
        load.start()
    fetched[0].wait()
    marked = (iota((n, tokens), 0) == tp_row[...]).astype(F32)
    before = (iota((tokens, tokens), 0) < iota((tokens, tokens), 1)).astype(F32)
    counted = dot(marked.astype(BF16), before.astype(BF16)) * marked
    rank_row = jnp.sum(counted, axis=0, keepdims=True).astype(jnp.int32)
    shape = (n * kvl * per, tokens)
    at = iota(shape, 0)
    hit = (at // (kvl * per) == tp_row[...]) & (lax.rem(at, per) == rank_row)
    spread = []
    for g in range(kvl):
        mark = (hit & (lax.rem(at // per, kvl) == g)).astype(F32).astype(BF16)
        spread.append(mark)
    fetched[1].wait()
    fetched[2].wait()
    q_parts = k_parts = v_parts = None
    for g in range(kvl):
        head = t * kvl + g
        q_part = dot(
            spread[g], queries[:, pl.ds(mult(head * group * HD, group * HD), group * HD)]
        )
        k_part = dot(spread[g], own_kv[:, pl.ds(mult(head * HD, HD), HD)])
        v_part = dot(spread[g], own_kv[:, pl.ds(mult(half_kv + head * HD, HD), HD)])
        q_parts = q_part if g == 0 else q_parts + q_part
        k_parts = k_part if g == 0 else k_parts + k_part
        v_parts = v_part if g == 0 else v_parts + v_part
    block = (n, kvl * per, HD)
    qsend[:, :, 0 : group * HD] = q_parts.astype(BF16).reshape(n, kvl * per, group * HD)
    qsend[:, :, group * HD : group * HD + HD] = k_parts.astype(BF16).reshape(block)
    qsend[:, :, group * HD + HD : block_cols] = v_parts.astype(BF16).reshape(block)

    fetched[3].wait()
    fetched[4].wait()
    lanes = meta.shape[2]
    at = iota((n * 8, tokens), 0)
    row = lax.rem(at, 8)
    wanted = jnp.where(row < experts_here, at // 8 * experts_here + row, -1)
    facts = jnp.where(row == experts_here, tp_row[...].astype(F32), 0.0)
    for k in range(ids.shape[0]):
        facts = facts + jnp.where(wanted == ids[k : k + 1, :], route_w[k : k + 1, :], 0.0)
    facts = jnp.concatenate([facts, jnp.zeros((n * 8, lanes - tokens), F32)], axis=1)
    msend[...] = facts.reshape(n, 8, lanes)

    pl.semaphore_wait(barrier, n)

    sends = []

    def go(copy):
        copy.start()
        sends.append(copy)

    for k in [*range(2, n), 1]:
        e = peer(k)
        go(remote(qsend.at[e], qrecv.at[me], q_ss.at[k], q_rs.at[me], e, t))
        go(remote(msend.at[e], meta.at[me], m_ss.at[k], m_rs.at[me], e, t))
    for i in range(2):
        go(
            remote(
                cache.at[0, :, pl.ds(mult(i * half_kv + ot * kvw, kvw), kvw)],
                kv.at[mine_at, pl.ds(i * kvw, kvw)],
                k_ss.at[i],
                k_rs.at[i],
                me,
                ot,
            )
        )
    for k in range(1, n):
        e = peer(k)
        go(
            remote(
                residual.at[:, pl.ds(mult(e * cols + t * hc, hc), hc)],
                resid.at[me],
                r_ss.at[k],
                r_rs.at[me],
                e,
                t,
            )
        )

    qrecv[me] = qsend[me]
    meta[me] = msend[me]
    for load in loads:
        load.start()
    for load in own_half:
        load.wait()
    fetched[5].wait()

    for k in range(1, n):
        e = peer(k)
        remote(meta.at[e], meta.at[e], m_ss.at[k], m_rs.at[e], e, t).wait_recv()

    slots = n * kvl * per
    place = iota((tokens, slots), 1)
    j = iota((tokens, slots), 0)
    base = jnp.zeros((1, 1), jnp.int32)
    pick = jnp.zeros((tokens, slots), F32)
    for s in range(n):
        names = meta[s, experts_here : experts_here + 1, 0:tokens].astype(jnp.int32)
        found = jnp.max((names == me).astype(F32), axis=1, keepdims=True)
        fits = (place // (kvl * per) == s) & (j == base + lax.rem(place, per))
        pick = pick + jnp.where(fits, found, 0.0)
        base = base + (found * per).astype(jnp.int32)
    for k in range(1, n):
        e = peer(k)
        remote(qsend.at[e], qrecv.at[e], q_ss.at[k], q_rs.at[e], e, t).wait_recv()
    for i in range(2):
        part = kv.at[pl.ds(mult(ot * span, span), span), pl.ds(i * kvw, kvw)]
        remote(part, part, k_ss.at[i], k_rs.at[i], me, ot).wait_recv()

    quarters = 2 * kvl
    quarter = heads_cols // quarters
    predicated = []

    def inside_line(zz):
        return (zz >= 0) & (zz < nz)

    def line_copy(off, q, way, at):
        b = (z + off) * 2 + c
        part = attn.at[slot(b), :, pl.ds(q * quarter, quarter)]
        return remote(
            part, part, a_ss.at[at], a_rs.at[slot(b) * quarters + q], (z + way) * 2 + c, t
        )

    def pass_line(off, q, way, at):
        pl.when(inside_line(z + way))(lambda: line_copy(off, q, way, at).start())
        predicated.append((off, way, functools.partial(line_copy, off, q, way, at)))

    def arrived(off, q):
        line_copy(off, q, 0, 0).wait_recv()

    def mate_copy(off, at):
        block = attn.at[slot((z + off) * 2 + c)]
        return remote(
            block, block, m_up_ss.at[at], m_up_rs.at[slot((z + off) * 2 + c)], mate, t
        )

    def to_mate(off, at):
        mate_copy(off, at).start()
        predicated.append((off, 0, functools.partial(mate_copy, off, at)))

    got = qrecv[...].reshape(slots, block_cols)
    positions = kv.shape[0]
    scale = HD ** (-0.5)
    inside = iota((1, positions), 1) < length[...]
    for g in range(kvl):
        chosen_rows = jnp.where(lax.rem(place // per, kvl) == g, pick, 0.0).astype(BF16)
        mine = dot(chosen_rows, got)
        q = jnp.concatenate([mine[:, i * HD : (i + 1) * HD] for i in range(group)], 0)
        k_own = jnp.concatenate([mine[:, group * HD : group * HD + HD]] * group, 0)
        v_own = jnp.concatenate([mine[:, group * HD + HD : block_cols]] * group, 0)
        keys = kv[:, g * HD : (g + 1) * HD]
        values = kv[:, kvw + g * HD : kvw + (g + 1) * HD]
        score = (
            lax.dot_general(
                q.astype(BF16), keys, (((1,), (1,)), ((), ())), preferred_element_type=F32
            )
            * scale
        )
        score = jnp.where(inside, score, MASKED_SCORE)
        own_score = jnp.sum(q * k_own, axis=1, keepdims=True) * scale
        top = jnp.maximum(jnp.max(score, axis=1, keepdims=True), own_score)
        weight = jnp.where(inside, jnp.exp(score - top), 0.0)
        own_weight = jnp.exp(own_score - top)
        bottom = jnp.sum(weight, axis=1, keepdims=True) + own_weight
        value = (dot(weight.astype(BF16), values) + own_weight * v_own) / bottom
        value = value.astype(BF16)
        for i in range(group):
            at_col = (g * group + i) * HD
            attn[slot(me), :, at_col : at_col + HD] = value[i * tokens : (i + 1) * tokens]
        for q in range(g * quarters // kvl, (g + 1) * quarters // kvl):
            pass_line(0, q, -1, q)
            pass_line(0, q, 1, quarters + q)
    to_mate(0, 0)

    info = meta[...].reshape(n * 8, lanes).T

    def column(r):
        return jnp.concatenate(
            [info[0:tokens, i * 8 + r : i * 8 + r + 1] for i in range(n)], axis=0
        )

    prompt = column(experts_here)
    wide = iota((everyone, lanes), 1)
    named = (prompt.astype(jnp.int32) == wide).astype(F32)
    square = (everyone, everyone)
    earlier = (iota(square, 1) < iota(square, 0)).astype(F32).astype(BF16)
    rank = jnp.sum(dot(earlier, named.astype(BF16)) * named, axis=1, keepdims=True)
    shifted = prompt + jnp.where(prompt < 2, n - 2, -2).astype(F32)
    row_at = (shifted * tokens + rank).astype(jnp.int32)
    chosen_at = (row_at == iota(square, 1)).astype(F32)
    perm[...] = chosen_at.astype(BF16)
    to_sorted = chosen_at.T.astype(BF16)
    spread_mix = jnp.zeros((everyone, lanes), F32)
    for x in range(experts_here):
        left = column(x)
        for i in range(3):
            piece = left.astype(BF16).astype(F32)
            left = left - piece
            spread_mix = spread_mix + jnp.where(wide == 3 * x + i, piece, 0.0)
    mixes[...] = dot(to_sorted, spread_mix.astype(BF16))

    def take(d):
        for q in range(quarters):
            for way in (1, -1):

                def land(q=q, way=way):
                    arrived(-way * d, q)
                    pass_line(-way * d, q, way, 2 * quarters * d + (quarters if way > 0 else 0) + q)

                pl.when(inside_line(z - way * d))(land)
        for way in (1, -1):

            def hand(way=way):
                to_mate(-way * d, 2 * d + (1 if way > 0 else 0))

            pl.when(inside_line(z - way * d))(hand)

    rows_a = (n - 4) * tokens
    stages = [(0, rows_a), (rows_a, everyone)]
    there = pl.ds(mult(ot * hc, hc), hc)
    here = pl.ds(mult(t * hc, hc), hc)

    def y_copy(st):
        rows = slice(*stages[st])
        return remote(
            ybuf.at[rows, there], yrecv.at[rows], y_ss.at[st], y_rs.at[st], me, ot
        )

    def project(st):
        first, last = stages[st]
        for at in range(first // (2 * tokens), last // (2 * tokens)):
            b = (at + 1) % nz * 2 + 1 - c
            block = attn.at[slot(b)]
            remote(block, block, m_up_ss.at[0], m_up_rs.at[slot(b)], mate, t).wait_recv()
        rows = slice(first, last)
        lhs = attn[first // tokens : last // tokens].reshape(last - first, heads_cols)
        ybuf[rows] = dot(lhs, wo[...]).astype(BF16)
        go(y_copy(st))

    def pass_on(st, b, half_at, k, e, tt):
        rows = slice(*stages[st])
        part = hidden.at[rows, pl.ds(mult(b * cols + half_at * hc, hc), hc)]
        at = 4 * nz * st + k
        go(remote(part, part, h_ss.at[at], h_rs.at[2 * n * st + 2 * b + half_at], e, tt))

    def arrives(st, b, half_at):
        rows = slice(*stages[st])
        part = hidden.at[rows, pl.ds(mult(b * cols + half_at * hc, hc), hc)]
        remote(
            part, part, h_ss.at[0], h_rs.at[2 * n * st + 2 * b + half_at], mate, t
        ).wait_recv()

    def finish(st):
        rows = slice(*stages[st])
        y_copy(st).wait_recv()
        hid = sorted_resid[rows].astype(F32) + (
            ybuf[rows, here].astype(F32) + yrecv[rows].astype(F32)
        )
        hidden[rows, pl.ds(mult(me * cols + t * hc, hc), hc)] = hid.astype(BF16)
        for k in range(1, nz):
            pass_on(st, me, t, k, zpeer(k), t)
        pass_on(st, me, t, nz, me, ot)
        pass_on(st, me, t, 0, mate, t)

    near_first = list(range(nz - 1, 0, -1))

    def relay_z(st):
        for k in near_first:
            b = zpeer(k)
            arrives(st, b, t)
            pass_on(st, b, t, nz + k, me, ot)
            pass_on(st, b, t, 2 * nz + k, mate, t)

    def relay_x(st):
        for k in [0, *near_first]:
            b = zpeer(k)
            arrives(st, b, ot)
            pass_on(st, b, ot, 3 * nz + k, mate, t)

    def from_mates(st):
        for k in [0, *near_first]:
            other = zline(k) * 2 + 1 - c
            arrives(st, other, t)
            arrives(st, other, ot)

    def expert(st):
        rows = slice(*stages[st])
        for x in range(experts_here):
            mix = mixes[rows, 3 * x : 3 * x + 1] + (
                mixes[rows, 3 * x + 1 : 3 * x + 2] + mixes[rows, 3 * x + 2 : 3 * x + 3]
            )
            gate = dot(hidden[rows], wg[x])
            value = gate / (1.0 + jnp.exp(-gate)) * dot(hidden[rows], wu[x]) * mix
            act[rows, x * ff : (x + 1) * ff] = value.astype(BF16)

    for d in range(1, nz - 1):
        take(d)
    loads[0].wait()
    project(0)
    take(nz - 1)
    project(1)
    for k in range(1, n):
        e = peer(k)
        remote(resid.at[e], resid.at[e], r_ss.at[k], r_rs.at[e], e, t).wait_recv()
    sorted_resid[...] = dot(to_sorted, resid[...].reshape(everyone, hc)).astype(BF16)
    finish(0)
    finish(1)
    relay_z(0)
    relay_z(1)
    relay_x(0)
    from_mates(0)
    loads[1].wait()
    loads[2].wait()
    expert(0)
    relay_x(1)
    from_mates(1)
    expert(1)
    loads[3].wait()
    there = pl.ds(mult(ot * half, half), half)
    here = pl.ds(mult(t * half, half), half)
    pair = 2 * tokens
    chunks = [(0, nz // 2), (nz // 2, nz)]

    def down(at_cols, at_sem, chunk):
        first, last = chunk
        rows = slice(first * pair, last * pair)
        part = None
        for x in range(experts_here):
            term = dot(own_act[rows, x * ff : (x + 1) * ff], wd[x, :, at_cols])
            part = term if part is None else part + term
        total[rows, at_cols] = part
        for zz in range(first, last):
            theirs = pl.ds(mult((zz * 2 + 1 - c) * tokens, tokens), tokens)
            dsend[zz, :, at_cols] = total[theirs, at_cols].astype(BF16)
            moved = dsend.at[zz, :, at_cols]
            dest = drecv.at[zz, :, at_cols]
            go(remote(moved, dest, d_ss.at[at_sem + zz], d_rs.at[at_sem + zz], mate, t))

    def from_mate(at_cols, at_sem, zz):
        dest = drecv.at[zz, :, at_cols]
        remote(dest, dest, d_ss.at[at_sem + zz], d_rs.at[at_sem + zz], mate, t).wait_recv()

    def ours(zz):
        return pl.ds(mult((zz * 2 + c) * tokens, tokens), tokens)

    def to_x(chunk):
        for zz in range(*chunk):
            from_mate(there, 0, zz)
            xsend[zz] = (total[ours(zz), there] + drecv[zz, :, there].astype(F32)).astype(BF16)
            go(remote(xsend.at[zz], xrecv.at[zz], x_ss.at[zz], x_rs.at[zz], me, ot))

    for i, chunk in enumerate(chunks):
        rows = slice(chunk[0] * pair, chunk[1] * pair)
        own_act[rows] = dot(perm[rows], act[...]).astype(BF16)
        down(there, 0, chunk)
    down(here, nz, chunks[0])
    to_x(chunks[0])
    down(here, nz, chunks[1])
    to_x(chunks[1])
    for zz in range(nz):
        from_mate(here, nz, zz)
        remote(xsend.at[zz], xrecv.at[zz], x_ss.at[zz], x_rs.at[zz], me, ot).wait_recv()
        done = total[ours(zz), here] + drecv[zz, :, here].astype(F32) + xrecv[zz].astype(F32)
        zsend[zz] = done.astype(BF16)
        total[ours(zz), here] = done

        def send_on(zz=zz):
            remote(
                zsend.at[zz], zrecv.at[z], z_ss.at[zz], z_rs.at[z], zz * 2 + c, t
            ).start()

        pl.when(z != zz)(send_on)
    own_rows = pl.ds(mult(me * tokens, tokens), tokens)
    final = total[own_rows, here] + dot(perm[own_rows], hidden[:, here])
    for off, way, copy in predicated:
        pl.when(inside_line(z + off) & inside_line(z + way))(lambda copy=copy: copy().wait_send())
    for copy in sends:
        copy.wait_send()
    for k in range(1, nz):
        zz = lax.rem(z + k, nz)
        remote(zrecv.at[zz], zrecv.at[zz], z_ss.at[0], z_rs.at[zz], zz * 2 + c, t).wait_recv()
        final = final + zrecv[zz].astype(F32)
    out[...] = final.astype(BF16)
    for zz in range(nz):

        def sent(zz=zz):
            remote(
                zsend.at[zz], zrecv.at[z], z_ss.at[zz], z_rs.at[z], zz * 2 + c, t
            ).wait_send()

        pl.when(z != zz)(sent)


def fused(
    queries,
    own_kv,
    prompt_cache,
    prompt_len,
    token_prompt,
    residual,
    out_weight,
    route_ids,
    route_weights,
    w_gate,
    w_up,
    w_down,
):
    n = lax.axis_size("expert")
    nz = n // 2
    tokens = queries.shape[0]
    per = tokens // nz
    kv_heads = own_kv.shape[1] // (2 * HD)
    group = queries.shape[1] // HD // kv_heads
    kvl = kv_heads // 2
    model = residual.shape[1]
    cols = model // n
    hc = cols // 2
    half = model // 2
    rows_per = kvl * per
    block_cols = group * HD + 2 * HD
    x_here, _, ff = w_gate.shape
    every = n * tokens
    sem = pltpu.SemaphoreType.DMA

    def vm(shape, kind=BF16):
        return pltpu.VMEM(shape, kind)

    vspec = pl.BlockSpec(memory_space=pltpu.VMEM)
    hspec = pl.BlockSpec(memory_space=pl.ANY)
    return pl.pallas_call(
        functools.partial(fused_kernel, (n, tokens, per, kvl, group)),
        out_shape=jax.ShapeDtypeStruct((tokens, half), BF16),
        in_specs=[hspec] * 12,
        out_specs=vspec,
        scratch_shapes=[
            vm(queries.shape),
            vm(own_kv.shape),
            vm((1, 1), jnp.int32),
            vm((1, tokens), jnp.int32),
            vm(route_ids.shape[::-1], jnp.int32),
            vm(route_weights.shape[::-1], F32),
            vm(out_weight.shape),
            vm(w_gate.shape),
            vm(w_up.shape),
            vm(w_down.shape),
            vm((n, rows_per, block_cols)),
            vm((n, rows_per, block_cols)),
            vm((2 * prompt_cache.shape[1], 2 * kvl * HD)),
            vm((n, 8, HD), F32),
            vm((n, 8, HD), F32),
            vm((n, tokens, cols // 2)),
            vm((every, cols // 2)),
            vm((every, every)),
            vm((every, HD), F32),
            vm((n, tokens, kvl * group * HD)),
            vm((every, cols)),
            vm((every, cols // 2)),
            vm((every, model)),
            vm((every, x_here * ff)),
            vm((every, x_here * ff)),
            vm((every, model), F32),
            vm((nz, tokens, model)),
            vm((nz, tokens, model)),
            vm((nz, tokens, half)),
            vm((nz, tokens, half)),
            vm((nz, tokens, half)),
            vm((nz, tokens, half)),
            sem((9,)),
            sem((4,)),
            sem((n,)),
            sem((n,)),
            sem((n,)),
            sem((n,)),
            sem((n,)),
            sem((n,)),
            sem((2,)),
            sem((2,)),
            sem((4 * kvl * nz,)),
            sem((2 * kvl * n,)),
            sem((2 * nz,)),
            sem((n,)),
            sem((2,)),
            sem((2,)),
            sem((8 * nz,)),
            sem((4 * n,)),
            sem((2 * nz,)),
            sem((2 * nz,)),
            sem((nz,)),
            sem((nz,)),
            sem((nz,)),
            sem((nz,)),
        ],
        compiler_params=pltpu.CompilerParams(
            collective_id=0, has_side_effects=True, vmem_limit_bytes=60 * 1024 * 1024
        ),
    )(
        queries,
        own_kv,
        prompt_cache,
        prompt_len.reshape(1, 1),
        token_prompt.reshape(1, tokens),
        residual,
        route_ids.T,
        route_weights.T,
        out_weight,
        w_gate,
        w_up,
        w_down,
    )


def chosen(*arrays):
    queries, own_kv, _, _, _, residual, _, _, _, w_gate, _, _ = arrays
    n = lax.axis_size("expert")
    tokens = queries.shape[0]
    kv_heads = own_kv.shape[1] // (2 * HD)
    fits = (
        lax.axis_size("tensor") == 2
        and n % 2 == 0
        and n >= 8
        and tokens % 16 == 0
        and tokens <= HD
        and tokens % (n // 2) == 0
        and kv_heads % 2 == 0
        and (kv_heads // 2) * (tokens // (n // 2)) % 16 == 0
        and residual.shape[1] % (2 * n * HD) == 0
        and w_gate.shape[0] < 8
        and 6 * w_gate.size + 24 * n * tokens * residual.shape[1] < 50 * 2**20
    )
    return fused(*arrays) if fits else local(*arrays)


def solution(mesh):
    in_specs = (
        P(("groups", "expert"), None),
        P(("groups", "expert"), None),
        P(("groups", "expert"), "tensor", None),
        P(("groups", "expert")),
        P(("groups", "expert")),
        P(("groups", "expert"), None),
        P("tensor", "expert"),
        P(("groups", "expert"), None),
        P(("groups", "expert"), None),
        P("expert", None, "tensor"),
        P("expert", None, "tensor"),
        P("expert", "tensor", None),
    )
    out_specs = P(("groups", "expert"), "tensor")
    return jax.shard_map(chosen, mesh=mesh, in_specs=in_specs, out_specs=out_specs, check_vma=False)
```
